256 devices in a mesh: band: 32 (over x_lo, z, core), ga: 8 (over y, x_hi).
Axes of the slice: x: 4 (x_hi: 2, x_lo: 2; x = x_hi * 2 + x_lo), y: 4, z: 8, core: 2. Of those that a mesh axis runs over, the one named last changes fastest.
Arguments:
- psi: float32 [2, 4096, 65536], P(None, 'band', 'ga'), may hold values from -0.0234375 to 0.0234375
- hx: float32 [2, 512, 65536], P(None, 'band', 'ga'), may hold values from -6 to 6
Outputs:
- h_sub: float32 [2, 4096, 512], P(None, ('band', 'ga'))
The draws below stay inside these ranges and needn't reach their ends.
All inputs are finite; a program needn't handle non-finite values.
Results may differ from the reference program's by a relative error of at most 0.00007.
Values sent between devices are 32-bit elements; how exact they have to be, the bound alone decides.
A program may use at most 128 MiB of HBM per device.

```python
import jax
import jax.numpy as jnp
from jax import lax

NB = 4096
NG = 65536
NBLK = 512


def level_of(stream_key, dims, shards, smallest, high):
    def one(position, shards_of):
        draws = jax.random.uniform(jax.random.fold_in(jax.random.fold_in(stream_key, 6), position), (shards_of,), jnp.float32, smallest / len(shards), high / len(shards))
        return jnp.repeat(jnp.exp(draws), dims[position] // shards_of).reshape((-1,) + (1,) * (len(dims) - position - 1))

    gain = one(*shards[0])
    for cut in shards[1:]:
        gain = gain * one(*cut)
    return gain


def gaussian(key, extent, scale, reach, split=(), held_as=jnp.bfloat16):
    factor_of = level_of(key, extent, split, -0.22, 0.18) if split else 1.0
    entries = jax.random.normal(key, extent, jnp.float32) * scale * factor_of
    return jnp.minimum(jnp.maximum(entries, -reach), reach).astype(held_as)


def setup_inputs(seed: int = 0) -> dict:
    key_list = jax.random.split(jax.random.key(seed), 3)
    psi = gaussian(key_list[0], (2, NB, NG), NG ** -0.5, 0.0234375, ((1, 32), (2, 8)), jnp.float32)
    hx = gaussian(key_list[1], (2, NBLK, NG), 1.0, 6.0, ((1, 32), (2, 8)), jnp.float32)
    return dict(psi=psi, hx=hx)


def contract(left, right):
    return lax.dot_general(left, right, (((1,), (1,)), ((), ())), precision=lax.Precision.HIGHEST, preferred_element_type=jnp.float32)


def reference(psi, hx):
    real_part = contract(psi[0], hx[0]) + contract(psi[1], hx[1])
    imag_part = contract(psi[0], hx[1]) - contract(psi[1], hx[0])
    return jnp.stack([real_part, imag_part], axis=0)
```

```python
import jax
import jax.numpy as jnp
from jax import lax
from jax.experimental import pallas as pl
from jax.experimental.pallas import tpu as pltpu
from jax.sharding import PartitionSpec as P

NZ = 8
NY = 4
N = 128
M = 16
NG = 8192
GC = 256
Q = 13
H = Q * GC
C = NG - 2 * H
GL = H + C
GROUPS = ((0, 2), (2, 7), (7, 11), (11, 13))
MESH = pl.DeviceIdType.MESH


def split(x):
    hi = x.astype(jnp.bfloat16)
    return hi, (x - hi.astype(jnp.float32)).astype(jnp.bfloat16)


def mm(left, right):
    return jnp.dot(left, right, preferred_element_type=jnp.float32)


def kernel(
    psi, hx, out,
    hb, lbh, lbc, pwh, pwl, pnh, pnl, nbst, ost, acc_o, acc_n, ys, yr, xt, xr,
    lsem, zss, zrs, dss, drs, xss, xrs, yss, yrs, fss, frs,
):
    b, a = lax.axis_index("band"), lax.axis_index("ga")
    c, z, xl = b % 2, (b // 2) % NZ, b // (2 * NZ)
    y, xh = a // 2, a % 2
    nb = 1 - xl

    def band(xl_, z_, c_):
        return (xl_ * NZ + z_) * 2 + c_

    to_x = (band(nb, z, c), a)
    to_core = (band(xl, z, 1 - c), a)
    to_z = ((band(xl, (z + 1) % NZ, c), a), (band(xl, (z + NZ - 1) % NZ, c), a))
    to_y = tuple((b, ((y + j) % NY) * 2 + xh) for j in range(1, NY))
    finals = ((1, 0), (0, 1), (1, 1))
    to_f = tuple((band((xl + i) % 2, z, c), y * 2 + (xh + j) % 2) for i, j in finals)

    def cols(which, length, start=0):
        return pl.ds(pl.multiple_of(which * H + start, 128), length)

    loads = [
        pltpu.make_async_copy(hx.at[:, :, cols(xl, H)], hb.at[z, xl, c, :, :, pl.ds(0, H)], lsem.at[0]),
        pltpu.make_async_copy(hx.at[:, :, pl.ds(2 * H, C)], hb.at[z, xl, c, :, :, pl.ds(H, C)], lsem.at[1]),
        pltpu.make_async_copy(psi.at[:, :, cols(xl, H)], ost.at[:, :, pl.ds(0, H)], lsem.at[2]),
        pltpu.make_async_copy(psi.at[:, :, pl.ds(2 * H, C)], ost.at[:, :, pl.ds(H, C)], lsem.at[3]),
    ]
    for load in loads:
        load.start()

    barrier = pltpu.get_barrier_semaphore()
    peers = (to_core,) + to_z + to_y + to_f
    for peer in peers:
        pl.semaphore_signal(barrier, inc=1, device_id=peer, device_id_type=MESH)
    pl.semaphore_wait(barrier, len(peers))

    sends = []

    def remote(src, dst, ss, rs, peer):
        return pltpu.make_async_remote_copy(
            src_ref=src, dst_ref=dst, send_sem=ss, recv_sem=rs, device_id=peer, device_id_type=MESH
        )

    def launch(copy):
        copy.start()
        sends.append(copy)

    def arrived(slot, ss, rs, peer):
        remote(slot, slot, ss, rs, peer).wait_recv()

    hx_parts = ((cols(nb, H), pl.ds(0, H)), (pl.ds(2 * H, C), pl.ds(H, C)))
    for i, (src, dst) in enumerate(hx_parts):
        launch(remote(hx.at[:, :, src], hb.at[z, xl, c, :, :, dst], xss.at[i], xrs.at[i], to_x))

    def send_psi(lo, hi):
        for q in range(lo, hi):
            launch(remote(psi.at[:, :, cols(nb, GC, q * GC)], nbst.at[q], xss.at[2 + q], xrs.at[2 + q], to_x))

    send_psi(0, 4)

    items = tuple((d, e, None) for d in range(3) for e in (0, 1)) + ((3, 0, 0), (3, 1, 0))

    def slot(s, e, half, core):
        ref = hb.at[s, (xl + e) % 2, core]
        return ref if half is None else ref.at[half]

    def place(way, d):
        return (z + (NZ - d if way == 0 else d)) % NZ

    def ring_item(way, i):
        d, e, half = items[i]
        return d, e, (None if half is None else way)

    def send_z(i):
        for way in (0, 1):
            d, e, half = ring_item(way, i)
            ref = slot(place(way, d), e, half, c)
            launch(remote(ref, ref, zss.at[way, i], zrs.at[way, i], to_z[way]))

    def wait_z(i):
        for way in (0, 1):
            d, e, half = ring_item(way, i)
            ref = slot(place(way, d + 1), e, half, c)
            arrived(ref, zss.at[way, i], zrs.at[way, i], to_z[way])

    def send_core(k, s, e, half=None):
        ref = slot(s, e, half, c)
        launch(remote(ref, ref, dss.at[k], drs.at[k], to_core))

    def wait_core(k, s, e, half=None):
        arrived(slot(s, e, half, 1 - c), dss.at[k], drs.at[k], to_core)

    def core_items(i):
        out_items = []
        for way in (0, 1):
            d, e, half = ring_item(way, i)
            out_items.append((2 + 2 * i + way, place(way, d + 1), e, half))
        return out_items

    def pass_on(i):
        for item in core_items(i):
            send_core(*item)

    def both_cores(i):
        for item in core_items(i):
            wait_core(*item)

    def turn(block, hi_ref, lo_ref, rows):
        for part in (0, 1):
            hi, lo = split(block(part).T)
            hi_ref[rows, part * N : (part + 1) * N] = hi
            lo_ref[rows, part * N : (part + 1) * N] = lo

    def prepare_own():
        @pl.loop(0, GL // GC)
        def _(k):
            rows = pl.ds(pl.multiple_of(k * GC, GC), GC)
            turn(lambda part: ost[part, :, rows], pwh, pwl, rows)

    def prepare_neighbour(lo, hi):
        for q in range(lo, hi):
            arrived(nbst.at[q], xss.at[2 + q], xrs.at[2 + q], to_x)

        @pl.loop(lo, hi)
        def _(q):
            rows = pl.ds(pl.multiple_of(q * GC, GC), GC)
            turn(lambda part: nbst[q, part], pnh, pnl, rows)

    R = 8 * M

    def convert(s):
        @pl.loop(0, H // GC)
        def _(k):
            at = pl.ds(pl.multiple_of(k * GC, GC), GC)
            hi, lo = split(hb[s, :, :, :, :, at].reshape(R, GC))
            lbh[s, 0:R, at] = hi
            lbh[s, R : 2 * R, at] = lo

        @pl.loop(0, C // GC)
        def _(k):
            at = pl.ds(pl.multiple_of(k * GC, GC), GC)
            src = pl.ds(pl.multiple_of(H + k * GC, GC), GC)
            hi, lo = split(hb[s, :, :, :, :, src].reshape(R, GC))
            lbc[0:R, at] = hi
            lbc[R : 2 * R, at] = lo

    def three(left, right_hi, right_lo):
        both = mm(left[...], right_hi[...])
        return both[:R] + both[R:] + mm(left[0:R, :], right_lo[...])

    def own(s):
        convert(s)
        acc_o[s] = three(lbh.at[s], pwh.at[0:H], pwl.at[0:H]) + three(lbc, pwh.at[H:GL], pwl.at[H:GL])

    def neighbour(s, lo, hi):
        k = slice(lo * GC, hi * GC)
        acc_n[s] += three(lbh.at[s, :, k], pnh.at[k], pnl.at[k])

    def over(lo, hi, body):
        @pl.loop(lo, hi)
        def _(i):
            body((z + NZ + i) % NZ)

    def pair(d, body):
        @pl.loop(0, 2)
        def _(i):
            body((z + NZ - d + 2 * d * i) % NZ)

    lane = lax.broadcasted_iota(jnp.int32, (4 * M, N), 1) // 32

    def y_copy(j, s):
        return remote(ys.at[(y + j) % NY, s], yr.at[j - 1, s], yss.at[j - 1, s], yrs.at[j - 1, s], to_y[j - 1])

    def share(s):
        v = []
        for acc in (acc_o, acc_n):
            t = acc[s].reshape(4, 2, M, 2 * N)
            v.append((t[:, 0, :, :N] + t[:, 1, :, N:]).reshape(4 * M, N))
            v.append((t[:, 1, :, :N] - t[:, 0, :, N:]).reshape(4 * M, N))
        for i in range(NY):
            piece = None
            for k in range(4):
                shift = (32 * (k - i)) % 128
                moved = pltpu.roll(v[k], shift, 1) if shift else v[k]
                piece = moved if piece is None else jnp.where(lane == k, moved, piece)
            ys[i, s] = piece
        for j in range(1, NY):
            y_copy(j, s).start()

    loads[0].wait()
    loads[1].wait()
    send_z(0)
    send_core(0, z, 0)
    acc_n[...] = jnp.zeros_like(acc_n)
    loads[2].wait()
    loads[3].wait()
    prepare_own()

    for i, (_, dst) in enumerate(hx_parts):
        arrived(hb.at[z, nb, c, :, :, dst], xss.at[i], xrs.at[i], to_x)
    send_z(1)
    send_core(1, z, 1)
    send_psi(4, 7)
    wait_z(0)
    send_z(2)
    pass_on(0)
    wait_core(0, z, 0)
    wait_core(1, z, 1)
    own(z)

    wait_z(1)
    send_z(3)
    pass_on(1)
    send_psi(7, 9)
    both_cores(0)
    both_cores(1)
    pair(1, own)
    prepare_neighbour(*GROUPS[0])
    over(-1, 2, lambda s: neighbour(s, *GROUPS[0]))

    wait_z(2)
    send_z(4)
    pass_on(2)
    send_psi(9, 11)
    wait_z(3)
    send_z(5)
    pass_on(3)
    send_psi(11, 13)
    both_cores(2)
    both_cores(3)
    pair(2, own)
    pair(2, lambda s: neighbour(s, *GROUPS[0]))
    prepare_neighbour(*GROUPS[1])
    over(-2, 3, lambda s: neighbour(s, *GROUPS[1]))

    wait_z(4)
    send_z(6)
    pass_on(4)
    wait_z(5)
    send_z(7)
    pass_on(5)
    both_cores(4)
    both_cores(5)
    pair(3, own)
    pair(3, lambda s: neighbour(s, 0, GROUPS[1][1]))
    prepare_neighbour(*GROUPS[2])
    over(-3, 4, lambda s: neighbour(s, *GROUPS[2]))
    prepare_neighbour(*GROUPS[3])

    def last_group(s):
        neighbour(s, *GROUPS[3])
        share(s)

    over(-3, 4, last_group)

    wait_z(6)
    pass_on(6)
    wait_z(7)
    pass_on(7)
    both_cores(6)
    both_cores(7)
    far = (z + 4) % NZ
    own(far)
    neighbour(far, 0, Q)
    share(far)

    @pl.loop(0, NZ)
    def _(s):
        for j in range(1, NY):
            y_copy(j, s).wait()

    for e in (0, 1):
        for quad in (0, 1):
            rows = []
            for s in range(quad * 4, quad * 4 + 4):
                at = pl.ds(e * 2 * M, 2 * M)
                rows.append(ys[y, s, at, :] + yr[0, s, at, :] + yr[1, s, at, :] + yr[2, s, at, :])
            block = jnp.concatenate(rows, axis=0).T
            m0 = e * 16 * NZ * 2 + quad * 128
            xt[:, :, :, :, m0 : m0 + 128] = block.reshape(2, 2, 2, M, 128)

    last = []
    for k, (i, j) in enumerate(finals):
        last.append(remote(xt.at[i, :, (xh + j) % 2], xr.at[k], fss.at[k], frs.at[k], to_f[k]))
        last[-1].start()
    total = xt[0, :, xh]
    for k, copy in enumerate(last):
        copy.wait_recv()
        total = total + xr[k]
    out[...] = total
    for copy in last + sends:
        copy.wait_send()


def per_device(psi, hx):
    f32, bf16, vmem, dma = jnp.float32, jnp.bfloat16, pltpu.VMEM, pltpu.SemaphoreType.DMA
    hbm = pl.BlockSpec(memory_space=pl.ANY)
    return pl.pallas_call(
        kernel,
        out_shape=jax.ShapeDtypeStruct((2, N // 8, 32 * M), f32),
        in_specs=[hbm, hbm],
        out_specs=pl.BlockSpec(memory_space=pltpu.VMEM),
        scratch_shapes=[
            vmem((NZ, 2, 2, 2, M, GL), f32),
            vmem((NZ, 16 * M, H), bf16),
            vmem((16 * M, C), bf16),
            vmem((GL, 2 * N), bf16),
            vmem((GL, 2 * N), bf16),
            vmem((H, 2 * N), bf16),
            vmem((H, 2 * N), bf16),
            vmem((Q, 2, N, GC), f32),
            vmem((2, N, GL), f32),
            vmem((NZ, 8 * M, 2 * N), f32),
            vmem((NZ, 8 * M, 2 * N), f32),
            vmem((NY, NZ, 4 * M, N), f32),
            vmem((NY - 1, NZ, 4 * M, N), f32),
            vmem((2, 2, 2, M, 32 * M), f32),
            vmem((3, 2, M, 32 * M), f32),
            dma((4,)),
            dma((2, 8)), dma((2, 8)),
            dma((18,)), dma((18,)),
            dma((2 + Q,)), dma((2 + Q,)),
            dma((NY - 1, NZ)), dma((NY - 1, NZ)),
            dma((3,)), dma((3,)),
        ],
        compiler_params=pltpu.CompilerParams(
            collective_id=0, has_side_effects=True, vmem_limit_bytes=66_000_000
        ),
    )(psi, hx)


def solution(mesh):
    in_specs = (P(None, "band", "ga"), P(None, "band", "ga"))
    out_specs = P(None, ("band", "ga"), None)
    return jax.shard_map(
        per_device, mesh=mesh, in_specs=in_specs, out_specs=out_specs, check_vma=False
    )
```

```python
import jax
import jax.numpy as jnp
from jax import lax
from jax.experimental import pallas as pl
from jax.experimental.pallas import tpu as pltpu
from jax.sharding import PartitionSpec as P

NZ = 8
NY = 4
N = 128
M = 16
NG = 8192
GC = 256
Q = 13
H = Q * GC
C = NG - 2 * H
GL = H + C
MESH = pl.DeviceIdType.MESH


def split(x):
    hi = x.astype(jnp.bfloat16)
    return hi, (x - hi.astype(jnp.float32)).astype(jnp.bfloat16)


def mm(left, right):
    return jnp.dot(left, right, preferred_element_type=jnp.float32)


def kernel(
    psi, hx, out,
    hb, lbh, lbc, pwh, pwl, pnh, pnl, nbst, ost, acc_o, acc_n, ys, yr, xt, xr,
    lsem, zss, zrs, dss, drs, xss, xrs, yss, yrs, fss, frs,
):
    b, a = lax.axis_index("band"), lax.axis_index("ga")
    c, z, xl = b % 2, (b // 2) % NZ, b // (2 * NZ)
    y, xh = a // 2, a % 2
    nb = 1 - xl

    def band(xl_, z_, c_):
        return (xl_ * NZ + z_) * 2 + c_

    to_x = (band(nb, z, c), a)
    to_core = (band(xl, z, 1 - c), a)
    to_z = ((band(xl, (z + 1) % NZ, c), a), (band(xl, (z + NZ - 1) % NZ, c), a))
    to_y = tuple((b, ((y + j) % NY) * 2 + xh) for j in range(1, NY))
    finals = ((1, 0), (0, 1), (1, 1))
    to_f = tuple((band((xl + i) % 2, z, c), y * 2 + (xh + j) % 2) for i, j in finals)

    def cols(which, length, start=0):
        return pl.ds(pl.multiple_of(which * H + start, 128), length)

    loads = [
        pltpu.make_async_copy(hx.at[:, :, cols(xl, H)], hb.at[z, xl, c, :, :, pl.ds(0, H)], lsem.at[0]),
        pltpu.make_async_copy(hx.at[:, :, pl.ds(2 * H, C)], hb.at[z, xl, c, :, :, pl.ds(H, C)], lsem.at[1]),
        pltpu.make_async_copy(psi.at[:, :, cols(xl, H)], ost.at[:, :, pl.ds(0, H)], lsem.at[2]),
        pltpu.make_async_copy(psi.at[:, :, pl.ds(2 * H, C)], ost.at[:, :, pl.ds(H, C)], lsem.at[3]),
    ]
    for load in loads:
        load.start()

    barrier = pltpu.get_barrier_semaphore()
    peers = (to_core,) + to_z + to_y + to_f
    for peer in peers:
        pl.semaphore_signal(barrier, inc=1, device_id=peer, device_id_type=MESH)
    pl.semaphore_wait(barrier, len(peers))

    sends = []

    def remote(src, dst, ss, rs, peer):
        return pltpu.make_async_remote_copy(
            src_ref=src, dst_ref=dst, send_sem=ss, recv_sem=rs, device_id=peer, device_id_type=MESH
        )

    def launch(copy):
        copy.start()
        sends.append(copy)

    def arrived(slot, ss, rs, peer):
        remote(slot, slot, ss, rs, peer).wait_recv()

    hx_parts = ((cols(nb, H), pl.ds(0, H)), (pl.ds(2 * H, C), pl.ds(H, C)))
    for i, (src, dst) in enumerate(hx_parts):
        launch(remote(hx.at[:, :, src], hb.at[z, xl, c, :, :, dst], xss.at[i], xrs.at[i], to_x))

    def send_psi(lo, hi):
        for q in range(lo, hi):
            launch(remote(psi.at[:, :, cols(nb, GC, q * GC)], nbst.at[q], xss.at[2 + q], xrs.at[2 + q], to_x))

    send_psi(0, 4)

    items = tuple((d, e, None) for d in range(3) for e in (0, 1)) + ((3, 0, 0), (3, 1, 0))

    def slot(s, e, half, core):
        ref = hb.at[s, (xl + e) % 2, core]
        return ref if half is None else ref.at[half]

    def place(way, d):
        return (z + (NZ - d if way == 0 else d)) % NZ

    def ring_item(way, i):
        d, e, half = items[i]
        return d, e, (None if half is None else way)

    def send_z(i):
        for way in (0, 1):
            d, e, half = ring_item(way, i)
            ref = slot(place(way, d), e, half, c)
            launch(remote(ref, ref, zss.at[way, i], zrs.at[way, i], to_z[way]))

    def wait_z(i):
        for way in (0, 1):
            d, e, half = ring_item(way, i)
            ref = slot(place(way, d + 1), e, half, c)
            arrived(ref, zss.at[way, i], zrs.at[way, i], to_z[way])

    def send_core(k, s, e, half=None):
        ref = slot(s, e, half, c)
        launch(remote(ref, ref, dss.at[k], drs.at[k], to_core))

    def wait_core(k, s, e, half=None):
        arrived(slot(s, e, half, 1 - c), dss.at[k], drs.at[k], to_core)

    def core_items(i):
        out_items = []
        for way in (0, 1):
            d, e, half = ring_item(way, i)
            out_items.append((2 + 2 * i + way, place(way, d + 1), e, half))
        return out_items

    def pass_on(i):
        for item in core_items(i):
            send_core(*item)

    def both_cores(i):
        for item in core_items(i):
            wait_core(*item)

    def turn(block, hi_ref, lo_ref, rows):
        for part in (0, 1):
            hi, lo = split(block(part).T)
            hi_ref[rows, part * N : (part + 1) * N] = hi
            lo_ref[rows, part * N : (part + 1) * N] = lo

    def prepare_own():
        @pl.loop(0, GL // GC)
        def _(k):
            rows = pl.ds(pl.multiple_of(k * GC, GC), GC)
            turn(lambda part: ost[part, :, rows], pwh, pwl, rows)

    def prepare_neighbour(lo, hi):
        for q in range(lo, hi):
            arrived(nbst.at[q], xss.at[2 + q], xrs.at[2 + q], to_x)

        @pl.loop(lo, hi)
        def _(q):
            rows = pl.ds(pl.multiple_of(q * GC, GC), GC)
            turn(lambda part: nbst[q, part], pnh, pnl, rows)

    R = 4 * M

    def convert(s, e):
        @pl.loop(0, H // GC)
        def _(k):
            at = pl.ds(pl.multiple_of(k * GC, GC), GC)
            hi, lo = split(hb[s, e, :, :, :, at].reshape(R, GC))
            lbh[s, 0, e, :, at] = hi
            lbh[s, 1, e, :, at] = lo

        @pl.loop(0, C // GC)
        def _(k):
            at = pl.ds(pl.multiple_of(k * GC, GC), GC)
            src = pl.ds(pl.multiple_of(H + k * GC, GC), GC)
            hi, lo = split(hb[s, e, :, :, :, src].reshape(R, GC))
            lbc[0:R, at] = hi
            lbc[R : 2 * R, at] = lo

    def three(both, hi, right_hi, right_lo):
        rows = hi.shape[0]
        first = mm(both, right_hi)
        return first[:rows] + first[rows:] + mm(hi, right_lo)

    def own(s, i):
        e = (xl + i) % 2
        convert(s, e)
        acc_o[s, e] = three(
            lbh[s, :, e].reshape(2 * R, H), lbh[s, 0, e], pwh[0:H], pwl[0:H]
        ) + three(lbc[...], lbc[0:R], pwh[H:GL], pwl[H:GL])

    def neighbour(s, lo, hi):
        k = slice(lo * GC, hi * GC)
        left = lbh[s, :, :, :, k].reshape(4 * R, (hi - lo) * GC)
        acc_n[s] += three(left, left[: 2 * R], pnh[k], pnl[k]).reshape(2, R, 2 * N)

    def over(d, body):
        @pl.loop(0, 2 * d + 1)
        def _(i):
            body((z + NZ - d + i) % NZ)

    def pair(d, body):
        @pl.loop(0, 2)
        def _(i):
            body((z + NZ - d + 2 * d * i) % NZ)

    def last_group(s):
        neighbour(s, 10, Q)
        share(1, s)

    lane = lax.broadcasted_iota(jnp.int32, (2 * M, N), 1) // 32

    def y_copy(t, j, s):
        return remote(
            ys.at[t, (y + j) % NY, s], yr.at[t, j - 1, s], yss.at[t, j - 1, s], yrs.at[t, j - 1, s], to_y[j - 1]
        )

    def share(t, s):
        acc = (acc_o, acc_n)[t]
        v = []
        for e in (0, 1):
            p = acc[s, e].reshape(2, 2, M, 2 * N)
            v.append((p[:, 0, :, :N] + p[:, 1, :, N:]).reshape(2 * M, N))
            v.append((p[:, 1, :, :N] - p[:, 0, :, N:]).reshape(2 * M, N))
        for i in range(NY):
            piece = None
            for k in range(4):
                shift = (32 * (k - i)) % 128
                moved = pltpu.roll(v[k], shift, 1) if shift else v[k]
                piece = moved if piece is None else jnp.where(lane == k, moved, piece)
            ys[t, i, s] = piece
        for j in range(1, NY):
            y_copy(t, j, s).start()

    loads[0].wait()
    loads[1].wait()
    send_z(0)
    send_core(0, z, 0)
    acc_n[...] = jnp.zeros_like(acc_n)
    loads[2].wait()
    loads[3].wait()
    prepare_own()

    for i, (_, dst) in enumerate(hx_parts):
        arrived(hb.at[z, nb, c, :, :, dst], xss.at[i], xrs.at[i], to_x)
    send_z(1)
    send_core(1, z, 1)
    send_psi(4, 7)
    wait_z(0)
    send_z(2)
    pass_on(0)
    wait_core(0, z, 0)
    own(z, 0)

    wait_z(1)
    send_z(3)
    pass_on(1)
    send_psi(7, 9)
    wait_core(1, z, 1)
    own(z, 1)
    share(0, z)
    both_cores(0)
    pair(1, lambda s: own(s, 0))

    wait_z(2)
    send_z(4)
    pass_on(2)
    send_psi(9, 11)
    both_cores(1)
    pair(1, lambda s: own(s, 1))
    pair(1, lambda s: share(0, s))
    prepare_neighbour(0, 4)
    over(1, lambda s: neighbour(s, 0, 4))

    wait_z(3)
    send_z(5)
    pass_on(3)
    send_psi(11, Q)
    both_cores(2)
    pair(2, lambda s: own(s, 0))
    prepare_neighbour(4, 6)
    over(1, lambda s: neighbour(s, 4, 6))

    wait_z(4)
    send_z(6)
    pass_on(4)
    both_cores(3)
    pair(2, lambda s: own(s, 1))
    pair(2, lambda s: share(0, s))
    pair(2, lambda s: neighbour(s, 0, 6))
    prepare_neighbour(6, 10)
    over(2, lambda s: neighbour(s, 6, 10))
    both_cores(4)
    pair(3, lambda s: own(s, 0))

    wait_z(5)
    send_z(7)
    pass_on(5)
    far = (z + 4) % NZ
    across = [remote(slot(far, e, None, c), slot(far, e, None, c), dss.at[14 + e], drs.at[14 + e], to_core) for e in (0, 1)]
    sends.extend(across)

    def finish(i):
        wait_z(6 + i)
        across[i].start()

    @pl.when(c == 1)
    def _():
        finish(0)

    both_cores(5)

    @pl.loop(0, 3)
    def _(it):
        final = it // 2
        s = (z + 5 - 2 * it + 3 * final) % NZ

        @pl.when(it == 2)
        def _():
            @pl.when(c == 1)
            def _():
                finish(1)

            over(2, last_group)

        @pl.loop(1 - final, 2)
        def _(i):
            for e in (0, 1):

                @pl.when((it == 2) & (i == e))
                def _():
                    @pl.when(c == 0)
                    def _():
                        finish(e)

                    wait_core(14 + e, far, e)

            own(s, i)

        share(0, s)

        @pl.when(it == 0)
        def _():
            prepare_neighbour(10, Q)

        neighbour(s, 0, Q)
        share(1, s)

    last = []
    for turn_ in (0, 1):
        quad = z // 4 if turn_ == 0 else 1 - z // 4

        @pl.loop(0, 4)
        def _(i):
            for t in (0, 1):
                for j in range(1, NY):
                    y_copy(t, j, quad * 4 + i).wait_recv()

        for t in (0, 1):
            rows = []
            for i in range(4):
                s = quad * 4 + i
                rows.append(ys[t, y, s] + yr[t, 0, s] + yr[t, 1, s] + yr[t, 2, s])
            block = jnp.concatenate(rows, axis=0).T.reshape(2, 2, 2, M, 128)
            for e in (0, 1):
                xt[turn_, t, :, :, :, e * 128 : (e + 1) * 128] = block[e]
        for k, (i, j) in enumerate(finals):
            copy = remote(
                xt.at[turn_, i, :, (xh + j) % 2], xr.at[turn_, k], fss.at[turn_, k], frs.at[turn_, k], to_f[k]
            )
            copy.start()
            last.append(copy)
    for turn_ in (0, 1):
        quad = z // 4 if turn_ == 0 else 1 - z // 4
        total = xt[turn_, 0, :, xh]
        for k in range(3):
            last[3 * turn_ + k].wait_recv()
            total = total + xr[turn_, k]
        for e in (0, 1):
            out[:, :, pl.ds(pl.multiple_of(e * 256 + quad * 128, 128), 128)] = total[:, :, e * 128 : (e + 1) * 128]

    @pl.loop(0, NZ)
    def _(s):
        for t in (0, 1):
            for j in range(1, NY):
                y_copy(t, j, s).wait_send()

    for copy in last + sends:
        copy.wait_send()


def per_device(psi, hx):
    f32, bf16, vmem, dma = jnp.float32, jnp.bfloat16, pltpu.VMEM, pltpu.SemaphoreType.DMA
    hbm = pl.BlockSpec(memory_space=pl.ANY)
    return pl.pallas_call(
        kernel,
        out_shape=pltpu.VMEM((2, N // 8, 32 * M), f32),
        in_specs=[hbm, hbm],
        out_specs=pl.BlockSpec(memory_space=pltpu.VMEM),
        scratch_shapes=[
            vmem((NZ, 2, 2, 2, M, GL), f32),
            vmem((NZ, 2, 2, 4 * M, H), bf16),
            vmem((8 * M, C), bf16),
            vmem((GL, 2 * N), bf16),
            vmem((GL, 2 * N), bf16),
            vmem((H, 2 * N), bf16),
            vmem((H, 2 * N), bf16),
            vmem((Q, 2, N, GC), f32),
            vmem((2, N, GL), f32),
            vmem((NZ, 2, 4 * M, 2 * N), f32),
            vmem((NZ, 2, 4 * M, 2 * N), f32),
            vmem((2, NY, NZ, 2 * M, N), f32),
            vmem((2, NY - 1, NZ, 2 * M, N), f32),
            vmem((2, 2, 2, 2, M, 16 * M), f32),
            vmem((2, 3, 2, M, 16 * M), f32),
            dma((4,)),
            dma((2, 8)), dma((2, 8)),
            dma((16,)), dma((16,)),
            dma((2 + Q,)), dma((2 + Q,)),
            dma((2, NY - 1, NZ)), dma((2, NY - 1, NZ)),
            dma((2, 3)), dma((2, 3)),
        ],
        compiler_params=pltpu.CompilerParams(
            collective_id=0, has_side_effects=True, vmem_limit_bytes=66_000_000
        ),
    )(psi, hx)


def solution(mesh):
    in_specs = (P(None, "band", "ga"), P(None, "band", "ga"))
    out_specs = P(None, ("band", "ga"), None)
    return jax.shard_map(
        per_device, mesh=mesh, in_specs=in_specs, out_specs=out_specs, check_vma=False
    )
```

```python
import jax
import jax.numpy as jnp
from jax import lax
from jax.experimental import pallas as pl
from jax.experimental.pallas import tpu as pltpu
from jax.sharding import PartitionSpec as P

NZ = 8
NY = 4
N = 128
M = 16
NG = 8192
GC = 128
Q = 26
CUTS = ((0, 14, Q), (0, 14, 20, Q))
PIECES = tuple(
    (2 * h + i, CUTS[h][p], CUTS[h][p + 1]) for h in (0, 1) for p in range(len(CUTS[h]) - 1) for i in (0, 1)
)
H = Q * GC
C = NG - 2 * H
GL = H + C
CC = GC * (2 - Q % 2)
U = N // NY
MESH = pl.DeviceIdType.MESH


def split(x):
    hi = x.astype(jnp.bfloat16)
    return hi, (x - hi.astype(jnp.float32)).astype(jnp.bfloat16)


def mm(left, right):
    return jnp.dot(left, right, preferred_element_type=jnp.float32)


def kernel(
    psi, hx, out,
    hb, lbh, lbc, pwh, pwl, pnh, pnl, nbst, ost, acc_o, acc_n, ys, yr, xt, xr,
    lsem, zss, zrs, dss, drs, xss, xrs, yss, yrs, fss, frs,
):
    b, a = lax.axis_index("band"), lax.axis_index("ga")
    c, z, xl = b % 2, (b // 2) % NZ, b // (2 * NZ)
    y, xh = a // 2, a % 2
    nb = 1 - xl

    def band(xl_, z_, c_):
        return (xl_ * NZ + z_) * 2 + c_

    to_x = (band(nb, z, c), a)
    to_core = (band(xl, z, 1 - c), a)
    to_z = ((band(xl, (z + 1) % NZ, c), a), (band(xl, (z + NZ - 1) % NZ, c), a))
    to_y = tuple((b, ((y + j) % NY) * 2 + xh) for j in range(1, NY))
    finals = ((1, 0), (0, 1), (1, 1))
    to_f = tuple((band((xl + i) % 2, z, c), y * 2 + (xh + j) % 2) for i, j in finals)

    def cols(which, length, start=0):
        return pl.ds(pl.multiple_of(which * H + start, 128), length)

    loads = [
        pltpu.make_async_copy(hx.at[:, :, cols(xl, H)], hb.at[z, xl, c, :, :, pl.ds(0, H)], lsem.at[0]),
        pltpu.make_async_copy(hx.at[:, :, pl.ds(2 * H, C)], hb.at[z, xl, c, :, :, pl.ds(H, C)], lsem.at[1]),
        pltpu.make_async_copy(psi.at[:, :, cols(xl, H)], ost.at[:, :, pl.ds(0, H)], lsem.at[2]),
        pltpu.make_async_copy(psi.at[:, :, pl.ds(2 * H, C)], ost.at[:, :, pl.ds(H, C)], lsem.at[3]),
    ]
    for load in loads:
        load.start()

    barrier = pltpu.get_barrier_semaphore()
    peers = (to_core,) + to_z + to_y + to_f
    for peer in peers:
        pl.semaphore_signal(barrier, inc=1, device_id=peer, device_id_type=MESH)
    pl.semaphore_wait(barrier, len(peers))

    def remote(src, dst, ss, rs, peer):
        return pltpu.make_async_remote_copy(
            src_ref=src, dst_ref=dst, send_sem=ss, recv_sem=rs, device_id=peer, device_id_type=MESH
        )

    def launch(copy):
        copy.start()

    def arrived(slot, ss, rs, peer):
        remote(slot, slot, ss, rs, peer).wait_recv()

    hx_parts = ((cols(nb, H), pl.ds(0, H)), (pl.ds(2 * H, C), pl.ds(H, C)))
    for i, (src, dst) in enumerate(hx_parts):
        launch(remote(hx.at[:, :, src], hb.at[z, xl, c, :, :, dst], xss.at[0], xrs.at[i], to_x))

    quarter = [pl.ds(pl.multiple_of(((y + 1 + i) % NY) * U, U), U) for i in range(NY)]

    def crossing(n):
        i, lo, hi = PIECES[n]
        at = pl.ds(lo * GC, (hi - lo) * GC)
        return remote(
            psi.at[:, quarter[i], cols(nb, (hi - lo) * GC, lo * GC)],
            nbst.at[i, :, :, at],
            xss.at[1],
            xrs.at[2 + n],
            to_x,
        )

    def send_psi(lo, hi):
        for n in range(lo, hi):
            launch(crossing(n))

    send_psi(0, 2)

    whole, inner, outer = pl.ds(0, GL), pl.ds(0, H), pl.ds(H, C)
    items = tuple((d, e, False, whole) for d in range(3) for e in (0, 1))
    items += ((3, 0, True, whole), (3, 1, True, inner), (3, 1, True, outer))

    def slot(s, e, core, at=whole):
        return hb.at[s, (xl + e) % 2, core, :, :, at]

    def place(way, d):
        return (z + (NZ - d if way == 0 else d)) % NZ

    def ring_item(way, i, hop):
        d, e, halved, at = items[i]
        ref = slot(place(way, d + hop), e, c, at)
        ref = ref.at[way] if halved else ref
        return remote(ref, ref, zss, zrs.at[way, i], to_z[way])

    def send_z(i):
        for way in (0, 1):
            launch(ring_item(way, i, 0))

    def wait_z(i):
        for way in (0, 1):
            ring_item(way, i, 1).wait_recv()

    def cross(k, s, e, at=whole):
        ref = slot(s, e, c, at)
        return remote(ref, ref, dss, drs.at[k], to_core)

    def send_core(*item):
        launch(cross(*item))

    def wait_core(k, s, e, at=whole):
        arrived(slot(s, e, 1 - c, at), dss, drs.at[k], to_core)

    def core_items(i):
        d, e, _, _ = items[i]
        return [(2 + 2 * i + way, place(way, d + 1), e) for way in (0, 1)]

    def pass_on(i):
        for item in core_items(i):
            send_core(*item)

    def both_cores(i):
        for item in core_items(i):
            wait_core(*item)

    def turn(rows, hi_ref, lo_ref, at):
        hi, lo = split(jnp.concatenate(rows, axis=0).T)
        hi_ref[at] = hi
        lo_ref[at] = lo

    def prepare_own():
        @pl.loop(0, GL // GC)
        def _(k):
            at = pl.ds(pl.multiple_of(k * GC, GC), GC)
            for h in (0, 1):
                rows = [ost[part, quarter[i], at] for i in (2 * h, 2 * h + 1) for part in (0, 1)]
                turn(rows, pwh, pwl, (at, slice(h * N, (h + 1) * N)))

    def prepare_neighbour(h, lo, hi):
        for n, (i, first, last) in enumerate(PIECES):
            if i // 2 == h and lo <= first and last <= hi:
                crossing(n).wait_recv()

        @pl.loop(lo, hi)
        def _(k):
            at = pl.ds(pl.multiple_of(k * GC, GC), GC)
            rows = [nbst[i, part, :, at] for i in (2 * h, 2 * h + 1) for part in (0, 1)]
            turn(rows, pnh, pnl, (at, slice(h * N, (h + 1) * N)))

    R = 4 * M

    def three(hi, lo, right_hi, right_lo):
        rows = hi.shape[0]
        first = mm(jnp.concatenate([hi, lo], axis=0), right_hi)
        return first[:rows] + first[rows:] + mm(hi, right_lo)

    def named(blocks):
        return [(s, (xl + i) % 2) for s, i in blocks]

    def own_inner(*blocks):
        blocks = named(blocks)
        for s, e in blocks:

            @pl.loop(0, H // CC)
            def _(i):
                at = pl.ds(pl.multiple_of(i * CC, CC), CC)
                hi, lo = split(hb[s, e, :, :, :, at].reshape(R, CC))
                lbh[s, 0, e, :, at] = hi
                lbh[s, 1, e, :, at] = lo

        hi, lo = (jnp.concatenate([lbh[s, w, e] for s, e in blocks], axis=0) for w in (0, 1))
        product = three(hi, lo, pwh[0:H], pwl[0:H])
        for k, (s, e) in enumerate(blocks):
            acc_o[s, e] = product[k * R : (k + 1) * R]

    def own_outer(*blocks):
        blocks = named(blocks)
        for k, (s, e) in enumerate(blocks):

            @pl.loop(0, C // CC)
            def _(i):
                at = pl.ds(pl.multiple_of(i * CC, CC), CC)
                src = pl.ds(pl.multiple_of(H + i * CC, CC), CC)
                hi, lo = split(hb[s, e, :, :, :, src].reshape(R, CC))
                lbc[0, k, :, at] = hi
                lbc[1, k, :, at] = lo

        hi, lo = (lbc[w, : len(blocks)].reshape(-1, C) for w in (0, 1))
        product = three(hi, lo, pwh[H:GL], pwl[H:GL])
        for k, (s, e) in enumerate(blocks):
            acc_o[s, e] += product[k * R : (k + 1) * R]

    def own(*blocks):
        own_inner(*blocks)
        own_outer(*blocks)

    lane = lax.broadcasted_iota(jnp.int32, (2 * M, N), 1)
    def every(s):
        left = [lbh[s, w].reshape(2 * R, H) for w in (0, 1)]
        acc_n[s] = three(*left, pnh[...], pnl[...]).reshape(2, R, 2 * N)

    def half(s, h, lo, hi):
        k, at = slice(lo * GC, hi * GC), slice(h * N, (h + 1) * N)
        left = [lbh[s, w, :, :, k].reshape(2 * R, -1) for w in (0, 1)]
        acc_n[s, :, :, at] += three(*left, pnh[k, at], pnl[k, at]).reshape(2, R, N)

    def over(d, body):
        @pl.loop(0, 2 * d + 1)
        def _(i):
            body((z + NZ - d + i) % NZ)

    def pair(d, body):
        @pl.loop(0, 2)
        def _(i):
            body((z + NZ - d + 2 * d * i) % NZ)

    def y_copy(t, i, s):
        return remote(ys.at[t, i, s], yr.at[t, i, s], yss, yrs.at[(s // 4 + z // 4) % 2], to_y[i])

    def share(t, s, quarters=range(NY)):
        acc = (acc_o, acc_n)[t]
        real = lane % (2 * U) < U
        for h in sorted({i // 2 for i in quarters}):
            v = []
            for e in (0, 1):
                p = acc[s, e, :, h * N : (h + 1) * N].reshape(2, 2, M, N)
                p0, p1 = (p[:, w].reshape(2 * M, N) for w in (0, 1))
                crossed = jnp.where(real, pltpu.roll(p1, N - U, 1), pltpu.roll(p1, U, 1))
                v.append(crossed + jnp.where(real, p0, -p0))
            for i in (2 * h, 2 * h + 1):
                if i not in quarters:
                    continue
                if i % 2 == 0:
                    ys[t, i, s] = jnp.where(lane < N // 2, v[0], pltpu.roll(v[1], N // 2, 1))
                else:
                    ys[t, i, s] = jnp.where(lane < N // 2, pltpu.roll(v[0], N // 2, 1), v[1])
        for i in quarters:
            if i < NY - 1:
                y_copy(t, i, s).start()

    loads[0].wait()
    loads[1].wait()
    send_z(0)
    send_core(0, z, 0)
    acc_n[...] = jnp.zeros_like(acc_n)
    loads[2].wait()
    loads[3].wait()
    prepare_own()

    for i, (_, dst) in enumerate(hx_parts):
        arrived(hb.at[z, nb, c, :, :, dst], xss.at[0], xrs.at[i], to_x)
    send_z(1)
    send_core(1, z, 1)
    send_psi(2, 4)
    wait_z(0)
    send_z(2)
    pass_on(0)

    wait_z(1)
    send_z(3)
    pass_on(1)
    send_psi(4, 5)
    wait_core(0, z, 0)
    wait_core(1, z, 1)
    own((z, 0), (z, 1))
    share(0, z)
    both_cores(0)
    own((place(0, 1), 0), (place(1, 1), 0))

    wait_z(2)
    send_z(4)
    pass_on(2)
    send_psi(5, 7)
    both_cores(1)
    own((place(0, 1), 1), (place(1, 1), 1))
    pair(1, lambda s: share(0, s))

    def first_half(s):
        half(s, 0, 0, Q)
        share(1, s, (0, 1))

    wait_z(3)
    send_z(5)
    pass_on(3)
    send_psi(7, len(PIECES))
    both_cores(2)
    own((place(0, 2), 0), (place(1, 2), 0))
    prepare_neighbour(0, 0, Q)
    over(1, first_half)

    wait_z(4)
    send_z(6)
    pass_on(4)
    both_cores(3)
    own((place(0, 2), 1), (place(1, 2), 1))
    pair(2, lambda s: share(0, s))
    pair(2, first_half)
    prepare_neighbour(1, 0, CUTS[1][1])
    over(2, lambda s: half(s, 1, 0, CUTS[1][1]))
    both_cores(4)
    own((place(0, 3), 0), (place(1, 3), 0))
    prepare_neighbour(1, CUTS[1][1], CUTS[1][2])
    over(2, lambda s: half(s, 1, CUTS[1][1], CUTS[1][2]))

    wait_z(5)
    send_z(7)
    send_z(8)
    pass_on(5)
    far = place(0, 4)
    last_items = ((14, far, 0), (15, far, 1, inner), (16, far, 1, outer))
    across = [cross(*item) for item in last_items]

    def finish(i):
        wait_z(6 + i)
        across[i].start()

    def on(core, *steps):
        @pl.when(c == core)
        def _():
            for step in steps:
                step()

    def at_turn(it, value, *steps):
        @pl.when(it == value)
        def _():
            for step in steps:
                step()

    def rest(s):
        half(s, 1, CUTS[1][2], Q)
        share(1, s, (2, 3))

    def end_of_psi():
        prepare_neighbour(1, CUTS[1][2], Q)
        over(2, rest)

    on(1, lambda: finish(0), end_of_psi)

    @pl.loop(0, 2)
    def _(it):
        blocks = ((jnp.where(it == 0, place(0, 3), far), 1 - it), (jnp.where(it == 0, place(1, 3), far), 1))

        def over_ready(body):
            @pl.loop(it, 2)
            def _(k):
                body(jnp.where(it == 1, far, jnp.where(k == 0, place(0, 3), place(1, 3))))

        def late(s):
            every(s)
            share(1, s)

        at_turn(it, 0, lambda: both_cores(5))
        at_turn(it, 1, lambda: on(1, lambda: finish(2)), *(lambda i=i: wait_core(*last_items[i]) for i in (0, 1)))
        own_inner(*blocks)
        at_turn(it, 0, lambda: on(0, end_of_psi, lambda: finish(0)))
        at_turn(it, 1, lambda: on(0, lambda: finish(2)))
        over_ready(late)
        at_turn(it, 0, lambda: finish(1))
        at_turn(it, 1, lambda: wait_core(*last_items[2]))
        own_outer(*blocks)
        over_ready(lambda s: share(0, s))

    for turn_ in (0, 1):
        quad = z // 4 if turn_ == 0 else 1 - z // 4

        arrived(yr.at[:, :, pl.ds(0, 4)], yss, yrs.at[turn_], to_y[0])

        for t in (0, 1):
            rows = []
            for i in range(4):
                s = quad * 4 + i
                rows.append(ys[t, NY - 1, s] + yr[t, 0, s] + yr[t, 1, s] + yr[t, 2, s])
            block = jnp.concatenate(rows, axis=0).T.reshape(2, 2, 2, M, 128)
            for e in (0, 1):
                xt[turn_, t, :, :, :, e * 128 : (e + 1) * 128] = block[e]
        for k, (i, j) in enumerate(finals):
            copy = remote(
                xt.at[turn_, i, :, (xh + j) % 2], xr.at[turn_, k], fss, frs.at[turn_], to_f[k]
            )
            copy.start()
    for turn_ in (0, 1):
        quad = z // 4 if turn_ == 0 else 1 - z // 4
        total = xt[turn_, 0, :, xh]
        arrived(xr.at[turn_], fss, frs.at[turn_], to_f[0])
        for k in range(3):
            total = total + xr[turn_, k]
        for e in (0, 1):
            out[:, :, pl.ds(pl.multiple_of(e * 256 + quad * 128, 128), 128)] = total[:, :, e * 128 : (e + 1) * 128]

    for ref, sem in (
        (hb.at[pl.ds(0, 7), 0], zss),
        (hb.at[:, 0], dss),
        (hb.at[0, 0, 0], xss.at[0]),
        (nbst, xss.at[1]),
        (yr, yss),
        (xr, fss),
    ):
        remote(ref, ref, sem, sem, to_x).wait_send()


def per_device(psi, hx):
    f32, bf16, vmem, dma = jnp.float32, jnp.bfloat16, pltpu.VMEM, pltpu.SemaphoreType.DMA
    hbm = pl.BlockSpec(memory_space=pl.ANY)
    return pl.pallas_call(
        kernel,
        out_shape=pltpu.VMEM((2, N // 8, 32 * M), f32),
        in_specs=[hbm, hbm],
        out_specs=pl.BlockSpec(memory_space=pltpu.VMEM),
        scratch_shapes=[
            vmem((NZ, 2, 2, 2, M, GL), f32),
            vmem((NZ, 2, 2, 4 * M, H), bf16),
            vmem((2, 2, 4 * M, C), bf16),
            vmem((GL, 2 * N), bf16),
            vmem((GL, 2 * N), bf16),
            vmem((H, 2 * N), bf16),
            vmem((H, 2 * N), bf16),
            vmem((NY, 2, U, H), f32),
            vmem((2, N, GL), f32),
            vmem((NZ, 2, 4 * M, 2 * N), f32),
            vmem((NZ, 2, 4 * M, 2 * N), f32),
            vmem((2, NY, NZ, 2 * M, N), f32),
            vmem((2, NY - 1, NZ, 2 * M, N), f32),
            vmem((2, 2, 2, 2, M, 16 * M), f32),
            vmem((2, 3, 2, M, 16 * M), f32),
            dma((4,)),
            dma, dma((2, 9)),
            dma, dma((17,)),
            dma((2,)), dma((2 + len(PIECES),)),
            dma, dma((2,)),
            dma, dma((2,)),
        ],
        compiler_params=pltpu.CompilerParams(
            collective_id=0, has_side_effects=True, vmem_limit_bytes=66_000_000
        ),
    )(psi, hx)


def solution(mesh):
    in_specs = (P(None, "band", "ga"), P(None, "band", "ga"))
    out_specs = P(None, ("band", "ga"), None)
    return jax.shard_map(
        per_device, mesh=mesh, in_specs=in_specs, out_specs=out_specs, check_vma=False
    )
```

```python
import jax
import jax.numpy as jnp
from jax import lax
from jax.experimental import pallas as pl
from jax.experimental.pallas import tpu as pltpu
from jax.sharding import PartitionSpec as P

NZ = 8
NY = 4
N = 128
M = 16
NG = 8192
GC = 128
Q = 26
CUTS = ((0, 14, Q), (0, 14, 20, Q))
PIECES = tuple(
    (2 * h + i, CUTS[h][p], CUTS[h][p + 1]) for h in (0, 1) for p in range(len(CUTS[h]) - 1) for i in (0, 1)
)
H = Q * GC
C = NG - 2 * H
GL = H + C
CC = GC * (2 - Q % 2)
U = N // NY
MESH = pl.DeviceIdType.MESH


def split(x):
    hi = x.astype(jnp.bfloat16)
    return hi, (x - hi.astype(jnp.float32)).astype(jnp.bfloat16)


def mm(left, right):
    return jnp.dot(left, right, preferred_element_type=jnp.float32)


def kernel(
    psi, hx, out,
    hb, lbh, lbc, pwh, pwl, pnh, pnl, nbst, ost, acc_o, acc_n, ys, yr, xt, xr,
    lsem, zss, zrs, dss, drs, xss, xrs, yss, yrs, fss, frs,
):
    b, a = lax.axis_index("band"), lax.axis_index("ga")
    c, z, xl = b % 2, (b // 2) % NZ, b // (2 * NZ)
    y, xh = a // 2, a % 2
    nb = 1 - xl

    def band(xl_, z_, c_):
        return (xl_ * NZ + z_) * 2 + c_

    to_x = (band(nb, z, c), a)
    to_core = (band(xl, z, 1 - c), a)
    to_z = ((band(xl, (z + 1) % NZ, c), a), (band(xl, (z + NZ - 1) % NZ, c), a))
    to_y = tuple((b, ((y + j) % NY) * 2 + xh) for j in range(1, NY))
    finals = ((0, 1), (1, 0), (1, 1))
    to_f = tuple((band((xl + i) % 2, z, c), y * 2 + (xh + j) % 2) for i, j in finals)

    def cols(which, length, start=0):
        return pl.ds(pl.multiple_of(which * H + start, 128), length)

    loads = [
        pltpu.make_async_copy(hx.at[:, :, cols(xl, H)], hb.at[z, xl, c, :, :, pl.ds(0, H)], lsem.at[0]),
        pltpu.make_async_copy(hx.at[:, :, pl.ds(2 * H, C)], hb.at[z, xl, c, :, :, pl.ds(H, C)], lsem.at[1]),
        pltpu.make_async_copy(psi.at[:, :, cols(xl, H)], ost.at[:, :, pl.ds(0, H)], lsem.at[2]),
        pltpu.make_async_copy(psi.at[:, :, pl.ds(2 * H, C)], ost.at[:, :, pl.ds(H, C)], lsem.at[3]),
    ]
    for load in loads:
        load.start()

    barrier = pltpu.get_barrier_semaphore()
    peers = (to_core,) + to_z + to_y + to_f
    for peer in peers:
        pl.semaphore_signal(barrier, inc=1, device_id=peer, device_id_type=MESH)
    pl.semaphore_wait(barrier, len(peers))

    def remote(src, dst, ss, rs, peer):
        return pltpu.make_async_remote_copy(
            src_ref=src, dst_ref=dst, send_sem=ss, recv_sem=rs, device_id=peer, device_id_type=MESH
        )

    def launch(copy):
        copy.start()

    def arrived(slot, ss, rs, peer):
        remote(slot, slot, ss, rs, peer).wait_recv()

    hx_parts = ((cols(nb, H), pl.ds(0, H)), (pl.ds(2 * H, C), pl.ds(H, C)))
    for i, (src, dst) in enumerate(hx_parts):
        launch(remote(hx.at[:, :, src], hb.at[z, xl, c, :, :, dst], xss.at[0], xrs.at[i], to_x))

    quarter = [pl.ds(pl.multiple_of(((y + 1 + i) % NY) * U, U), U) for i in range(NY)]

    def crossing(n):
        i, lo, hi = PIECES[n]
        at = pl.ds(lo * GC, (hi - lo) * GC)
        return remote(
            psi.at[:, quarter[i], cols(nb, (hi - lo) * GC, lo * GC)],
            nbst.at[i, :, :, at],
            xss.at[1],
            xrs.at[2 + n],
            to_x,
        )

    def send_psi(lo, hi):
        for n in range(lo, hi):
            launch(crossing(n))

    send_psi(0, 2)

    whole, inner, outer = pl.ds(0, GL), pl.ds(0, H), pl.ds(H, C)
    items = tuple((d, e, False, whole) for d in range(3) for e in (0, 1))
    items += ((3, 0, True, whole), (3, 1, True, inner), (3, 1, True, outer))

    def slot(s, e, core, at=whole):
        return hb.at[s, (xl + e) % 2, core, :, :, at]

    def place(way, d):
        return (z + (NZ - d if way == 0 else d)) % NZ

    def ring_item(way, i, hop):
        d, e, halved, at = items[i]
        ref = slot(place(way, d + hop), e, c, at)
        ref = ref.at[way] if halved else ref
        return remote(ref, ref, zss, zrs.at[way, i], to_z[way])

    def send_z(i):
        for way in (0, 1):
            launch(ring_item(way, i, 0))

    def wait_z(i):
        for way in (0, 1):
            ring_item(way, i, 1).wait_recv()

    def cross(k, s, e, at=whole):
        ref = slot(s, e, c, at)
        return remote(ref, ref, dss, drs.at[k], to_core)

    def send_core(*item):
        launch(cross(*item))

    def wait_core(k, s, e, at=whole):
        arrived(slot(s, e, 1 - c, at), dss, drs.at[k], to_core)

    def core_items(i):
        d, e, _, _ = items[i]
        return [(2 + 2 * i + way, place(way, d + 1), e) for way in (0, 1)]

    def pass_on(i):
        for item in core_items(i):
            send_core(*item)

    def both_cores(i):
        for item in core_items(i):
            wait_core(*item)

    def turn(rows, hi_ref, lo_ref, at):
        hi, lo = split(jnp.concatenate(rows, axis=0).T)
        hi_ref[at] = hi
        lo_ref[at] = lo

    def prepare_own():
        @pl.loop(0, GL // GC)
        def _(k):
            at = pl.ds(pl.multiple_of(k * GC, GC), GC)
            for h in (0, 1):
                rows = [ost[part, quarter[i], at] for i in (2 * h, 2 * h + 1) for part in (0, 1)]
                turn(rows, pwh, pwl, (at, slice(h * N, (h + 1) * N)))

    def prepare_neighbour(h, lo, hi):
        for n, (i, first, last) in enumerate(PIECES):
            if i // 2 == h and lo <= first and last <= hi:
                crossing(n).wait_recv()

        @pl.loop(lo, hi)
        def _(k):
            at = pl.ds(pl.multiple_of(k * GC, GC), GC)
            rows = [nbst[i, part, :, at] for i in (2 * h, 2 * h + 1) for part in (0, 1)]
            turn(rows, pnh, pnl, (at, slice(h * N, (h + 1) * N)))

    R = 4 * M

    def three(hi, lo, right_hi, right_lo):
        rows = hi.shape[0]
        first = mm(jnp.concatenate([hi, lo], axis=0), right_hi)
        return first[:rows] + first[rows:] + mm(hi, right_lo)

    def named(blocks):
        return [(s, (xl + i) % 2) for s, i in blocks]

    def own_inner(*blocks):
        blocks = named(blocks)
        for s, e in blocks:

            @pl.loop(0, H // CC)
            def _(i):
                at = pl.ds(pl.multiple_of(i * CC, CC), CC)
                hi, lo = split(hb[s, e, :, :, :, at].reshape(R, CC))
                lbh[s, 0, e, :, at] = hi
                lbh[s, 1, e, :, at] = lo

        hi, lo = (jnp.concatenate([lbh[s, w, e] for s, e in blocks], axis=0) for w in (0, 1))
        product = three(hi, lo, pwh[0:H], pwl[0:H])
        for k, (s, e) in enumerate(blocks):
            acc_o[s, e] = product[k * R : (k + 1) * R]

    def own_outer(*blocks):
        blocks = named(blocks)
        for k, (s, e) in enumerate(blocks):

            @pl.loop(0, C // CC)
            def _(i):
                at = pl.ds(pl.multiple_of(i * CC, CC), CC)
                src = pl.ds(pl.multiple_of(H + i * CC, CC), CC)
                hi, lo = split(hb[s, e, :, :, :, src].reshape(R, CC))
                lbc[0, k, :, at] = hi
                lbc[1, k, :, at] = lo

        hi, lo = (lbc[w, : len(blocks)].reshape(-1, C) for w in (0, 1))
        product = three(hi, lo, pwh[H:GL], pwl[H:GL])
        for k, (s, e) in enumerate(blocks):
            acc_o[s, e] += product[k * R : (k + 1) * R]

    def own(*blocks):
        own_inner(*blocks)
        own_outer(*blocks)

    lane = lax.broadcasted_iota(jnp.int32, (2 * M, N), 1)
    def every(s):
        left = [lbh[s, w].reshape(2 * R, H) for w in (0, 1)]
        acc_n[s] = three(*left, pnh[...], pnl[...]).reshape(2, R, 2 * N)

    def half(s, h, lo, hi):
        k, at = slice(lo * GC, hi * GC), slice(h * N, (h + 1) * N)
        left = [lbh[s, w, :, :, k].reshape(2 * R, -1) for w in (0, 1)]
        acc_n[s, :, :, at] += three(*left, pnh[k, at], pnl[k, at]).reshape(2, R, N)

    def over(d, body):
        @pl.loop(0, 2 * d + 1)
        def _(i):
            body((z + NZ - d + i) % NZ)

    def pair(d, body):
        @pl.loop(0, 2)
        def _(i):
            body((z + NZ - d + 2 * d * i) % NZ)

    def y_copy(t, i, s):
        return remote(ys.at[t, i, s], yr.at[t, i, s], yss, yrs.at[(s // 4 + z // 4) % 2], to_y[i])

    def share(t, s, quarters=range(NY)):
        acc = (acc_o, acc_n)[t]
        real = lane % (2 * U) < U
        for h in sorted({i // 2 for i in quarters}):
            v = []
            for e in (0, 1):
                p = acc[s, e, :, h * N : (h + 1) * N].reshape(2, 2, M, N)
                p0, p1 = (p[:, w].reshape(2 * M, N) for w in (0, 1))
                crossed = jnp.where(real, pltpu.roll(p1, N - U, 1), pltpu.roll(p1, U, 1))
                v.append(crossed + jnp.where(real, p0, -p0))
            for i in (2 * h, 2 * h + 1):
                if i not in quarters:
                    continue
                if i % 2 == 0:
                    ys[t, i, s] = jnp.where(lane < N // 2, v[0], pltpu.roll(v[1], N // 2, 1))
                else:
                    ys[t, i, s] = jnp.where(lane < N // 2, pltpu.roll(v[0], N // 2, 1), v[1])
        for i in (1, 0, 2):
            if i in quarters:
                y_copy(t, i, s).start()

    loads[0].wait()
    loads[1].wait()
    send_z(0)
    send_core(0, z, 0)
    acc_n[...] = jnp.zeros_like(acc_n)
    loads[2].wait()
    loads[3].wait()
    prepare_own()

    for i, (_, dst) in enumerate(hx_parts):
        arrived(hb.at[z, nb, c, :, :, dst], xss.at[0], xrs.at[i], to_x)
    send_z(1)
    send_core(1, z, 1)
    send_psi(2, 4)
    wait_z(0)
    send_z(2)
    pass_on(0)

    wait_z(1)
    send_z(3)
    pass_on(1)
    send_psi(4, 5)
    wait_core(0, z, 0)
    wait_core(1, z, 1)
    own((z, 0), (z, 1))
    share(0, z)
    both_cores(0)
    own((place(0, 1), 0), (place(1, 1), 0))

    wait_z(2)
    send_z(4)
    pass_on(2)
    send_psi(5, 7)
    both_cores(1)
    own((place(0, 1), 1), (place(1, 1), 1))
    pair(1, lambda s: share(0, s))

    def first_half(s):
        half(s, 0, 0, Q)
        share(1, s, (0, 1))

    wait_z(3)
    send_z(5)
    pass_on(3)
    send_psi(7, len(PIECES))
    both_cores(2)
    own((place(0, 2), 0), (place(1, 2), 0))
    prepare_neighbour(0, 0, Q)
    over(1, first_half)

    wait_z(4)
    send_z(6)
    pass_on(4)
    both_cores(3)
    own((place(0, 2), 1), (place(1, 2), 1))
    pair(2, lambda s: share(0, s))
    pair(2, first_half)
    prepare_neighbour(1, 0, CUTS[1][1])
    over(2, lambda s: half(s, 1, 0, CUTS[1][1]))
    both_cores(4)
    own((place(0, 3), 0), (place(1, 3), 0))
    prepare_neighbour(1, CUTS[1][1], CUTS[1][2])
    over(2, lambda s: half(s, 1, CUTS[1][1], CUTS[1][2]))

    wait_z(5)
    send_z(7)
    send_z(8)
    pass_on(5)
    far = place(0, 4)
    last_items = ((14, far, 0), (15, far, 1, inner), (16, far, 1, outer))
    across = [cross(*item) for item in last_items]

    def finish(i):
        wait_z(6 + i)
        across[i].start()

    def on(core, *steps):
        @pl.when(c == core)
        def _():
            for step in steps:
                step()

    def at_turn(it, value, *steps):
        @pl.when(it == value)
        def _():
            for step in steps:
                step()

    def rest(s):
        half(s, 1, CUTS[1][2], Q)
        share(1, s, (2, 3))

    def end_of_psi():
        prepare_neighbour(1, CUTS[1][2], Q)
        over(2, rest)

    on(1, lambda: finish(0), end_of_psi)

    @pl.loop(0, 2)
    def _(it):
        blocks = ((jnp.where(it == 0, place(0, 3), far), 1 - it), (jnp.where(it == 0, place(1, 3), far), 1))

        def over_ready(body):
            @pl.loop(it, 2)
            def _(k):
                body(jnp.where(it == 1, far, jnp.where(k == 0, place(0, 3), place(1, 3))))

        def late(s):
            every(s)
            share(1, s)

        at_turn(it, 0, lambda: both_cores(5))
        at_turn(it, 1, lambda: on(1, lambda: finish(2)), *(lambda i=i: wait_core(*last_items[i]) for i in (0, 1)))
        own_inner(*blocks)
        at_turn(it, 0, lambda: on(0, end_of_psi, lambda: finish(0)))
        at_turn(it, 1, lambda: on(0, lambda: finish(2)))
        over_ready(late)
        at_turn(it, 0, lambda: on(1, lambda: finish(1)))
        at_turn(it, 1, lambda: wait_core(*last_items[2]))
        own_outer(*blocks)
        at_turn(it, 0, lambda: on(0, lambda: finish(1)))
        over_ready(lambda s: share(0, s))

    for turn_ in (0, 1):
        quad = z // 4 if turn_ == 0 else 1 - z // 4

        arrived(yr.at[:, :, pl.ds(0, 4)], yss, yrs.at[turn_], to_y[0])

        for t in (0, 1):
            rows = []
            for i in range(4):
                s = quad * 4 + i
                rows.append(ys[t, NY - 1, s] + yr[t, 0, s] + yr[t, 1, s] + yr[t, 2, s])
            block = jnp.concatenate(rows, axis=0).T.reshape(2, 2, 2, M, 128)
            for e in (0, 1):
                xt[turn_, t, :, :, :, e * 128 : (e + 1) * 128] = block[e]
        for k, (i, j) in enumerate(finals):
            copy = remote(
                xt.at[turn_, i, :, (xh + j) % 2], xr.at[turn_, k], fss, frs.at[turn_], to_f[k]
            )
            copy.start()
    for turn_ in (0, 1):
        quad = z // 4 if turn_ == 0 else 1 - z // 4
        total = xt[turn_, 0, :, xh]
        arrived(xr.at[turn_], fss, frs.at[turn_], to_f[0])
        for k in range(3):
            total = total + xr[turn_, k]
        for e in (0, 1):
            out[:, :, pl.ds(pl.multiple_of(e * 256 + quad * 128, 128), 128)] = total[:, :, e * 128 : (e + 1) * 128]

    for ref, sem in (
        (hb.at[pl.ds(0, 7), 0], zss),
        (hb.at[:, 0], dss),
        (hb.at[0, 0, 0], xss.at[0]),
        (nbst, xss.at[1]),
        (yr, yss),
        (xr, fss),
    ):
        remote(ref, ref, sem, sem, to_x).wait_send()


def per_device(psi, hx):
    f32, bf16, vmem, dma = jnp.float32, jnp.bfloat16, pltpu.VMEM, pltpu.SemaphoreType.DMA
    hbm = pl.BlockSpec(memory_space=pl.ANY)
    return pl.pallas_call(
        kernel,
        out_shape=pltpu.VMEM((2, N // 8, 32 * M), f32),
        in_specs=[hbm, hbm],
        out_specs=pl.BlockSpec(memory_space=pltpu.VMEM),
        scratch_shapes=[
            vmem((NZ, 2, 2, 2, M, GL), f32),
            vmem((NZ, 2, 2, 4 * M, H), bf16),
            vmem((2, 2, 4 * M, C), bf16),
            vmem((GL, 2 * N), bf16),
            vmem((GL, 2 * N), bf16),
            vmem((H, 2 * N), bf16),
            vmem((H, 2 * N), bf16),
            vmem((NY, 2, U, H), f32),
            vmem((2, N, GL), f32),
            vmem((NZ, 2, 4 * M, 2 * N), f32),
            vmem((NZ, 2, 4 * M, 2 * N), f32),
            vmem((2, NY, NZ, 2 * M, N), f32),
            vmem((2, NY - 1, NZ, 2 * M, N), f32),
            vmem((2, 2, 2, 2, M, 16 * M), f32),
            vmem((2, 3, 2, M, 16 * M), f32),
            dma((4,)),
            dma, dma((2, 9)),
            dma, dma((17,)),
            dma((2,)), dma((2 + len(PIECES),)),
            dma, dma((2,)),
            dma, dma((2,)),
        ],
        compiler_params=pltpu.CompilerParams(
            collective_id=0, has_side_effects=True, vmem_limit_bytes=66_000_000
        ),
    )(psi, hx)


def solution(mesh):
    in_specs = (P(None, "band", "ga"), P(None, "band", "ga"))
    out_specs = P(None, ("band", "ga"), None)
    return jax.shard_map(
        per_device, mesh=mesh, in_specs=in_specs, out_specs=out_specs, check_vma=False
    )
```

```python
import jax
import jax.numpy as jnp
from jax import lax
from jax.experimental import pallas as pl
from jax.experimental.pallas import tpu as pltpu
from jax.sharding import PartitionSpec as P

NZ = 8
NY = 4
N = 128
M = 16
NG = 8192
GC = 128
Q = 26
CUTS = ((0, 14, Q), (0, 14, 20, Q))
PIECES = tuple(
    (2 * h + i, CUTS[h][p], CUTS[h][p + 1]) for h in (0, 1) for p in range(len(CUTS[h]) - 1) for i in (0, 1)
)
H = Q * GC
C = NG - 2 * H
GL = H + C
CC = GC * (2 - Q % 2)
U = N // NY
MESH = pl.DeviceIdType.MESH


def split(x):
    hi = x.astype(jnp.bfloat16)
    return hi, (x - hi.astype(jnp.float32)).astype(jnp.bfloat16)


def mm(left, right):
    return jnp.dot(left, right, preferred_element_type=jnp.float32)


def kernel(
    psi, hx, out,
    hb, lbh, lbc, pwh, pwl, pnh, pnl, nbst, ost, acc_o, acc_n, ys, yr, xt, xr,
    lsem, zss, zrs, dss, drs, xss, xrs, yss, yrs, fss, frs,
):
    b, a = lax.axis_index("band"), lax.axis_index("ga")
    c, z, xl = b % 2, (b // 2) % NZ, b // (2 * NZ)
    y, xh = a // 2, a % 2
    nb = 1 - xl

    def band(xl_, z_, c_):
        return (xl_ * NZ + z_) * 2 + c_

    to_x = (band(nb, z, c), a)
    to_core = (band(xl, z, 1 - c), a)
    to_z = ((band(xl, (z + 1) % NZ, c), a), (band(xl, (z + NZ - 1) % NZ, c), a))
    to_y = tuple((b, ((y + j) % NY) * 2 + xh) for j in range(1, NY))
    finals = ((0, 1), (1, 0), (1, 1))
    to_f = tuple((band((xl + i) % 2, z, c), y * 2 + (xh + j) % 2) for i, j in finals)

    def cols(which, length, start=0):
        return pl.ds(pl.multiple_of(which * H + start, 128), length)

    loads = [
        pltpu.make_async_copy(hx.at[:, :, cols(xl, H)], hb.at[z, xl, c, :, :, pl.ds(0, H)], lsem.at[0]),
        pltpu.make_async_copy(hx.at[:, :, pl.ds(2 * H, C)], hb.at[z, xl, c, :, :, pl.ds(H, C)], lsem.at[1]),
        pltpu.make_async_copy(psi.at[:, :, cols(xl, H)], ost.at[:, :, pl.ds(0, H)], lsem.at[2]),
        pltpu.make_async_copy(psi.at[:, :, pl.ds(2 * H, C)], ost.at[:, :, pl.ds(H, C)], lsem.at[3]),
    ]
    for load in loads:
        load.start()

    barrier = pltpu.get_barrier_semaphore()
    peers = (to_core,) + to_z + to_y + to_f
    for peer in peers:
        pl.semaphore_signal(barrier, inc=1, device_id=peer, device_id_type=MESH)
    pl.semaphore_wait(barrier, len(peers))

    def remote(src, dst, ss, rs, peer):
        return pltpu.make_async_remote_copy(
            src_ref=src, dst_ref=dst, send_sem=ss, recv_sem=rs, device_id=peer, device_id_type=MESH
        )

    def launch(copy):
        copy.start()

    def arrived(slot, ss, rs, peer):
        remote(slot, slot, ss, rs, peer).wait_recv()

    hx_parts = ((cols(nb, H), pl.ds(0, H)), (pl.ds(2 * H, C), pl.ds(H, C)))
    for i, (src, dst) in enumerate(hx_parts):
        launch(remote(hx.at[:, :, src], hb.at[z, xl, c, :, :, dst], xss.at[0], xrs.at[i], to_x))

    quarter = [pl.ds(pl.multiple_of(((y + 1 + i) % NY) * U, U), U) for i in range(NY)]

    def crossing(n):
        i, lo, hi = PIECES[n]
        at = pl.ds(lo * GC, (hi - lo) * GC)
        return remote(
            psi.at[:, quarter[i], cols(nb, (hi - lo) * GC, lo * GC)],
            nbst.at[i, :, :, at],
            xss.at[1],
            xrs.at[2 + n],
            to_x,
        )

    def send_psi(lo, hi):
        for n in range(lo, hi):
            launch(crossing(n))

    send_psi(0, 2)

    whole, inner, outer = pl.ds(0, GL), pl.ds(0, H), pl.ds(H, C)
    items = tuple((d, e, False, whole) for d in range(3) for e in (0, 1))
    items += ((3, 0, True, whole), (3, 1, True, inner), (3, 1, True, outer))

    def slot(s, e, core, at=whole):
        return hb.at[s, (xl + e) % 2, core, :, :, at]

    def place(way, d):
        return (z + (NZ - d if way == 0 else d)) % NZ

    def ring_item(way, i, hop):
        d, e, halved, at = items[i]
        ref = slot(place(way, d + hop), e, c, at)
        ref = ref.at[way] if halved else ref
        return remote(ref, ref, zss, zrs.at[way, i], to_z[way])

    def send_z(i):
        for way in (0, 1):
            launch(ring_item(way, i, 0))

    def wait_z(i):
        for way in (0, 1):
            ring_item(way, i, 1).wait_recv()

    def cross(k, s, e, at=whole):
        ref = slot(s, e, c, at)
        return remote(ref, ref, dss, drs.at[k], to_core)

    def send_core(*item):
        launch(cross(*item))

    def wait_core(k, s, e, at=whole):
        arrived(slot(s, e, 1 - c, at), dss, drs.at[k], to_core)

    def core_items(i):
        d, e, _, _ = items[i]
        return [(2 + 2 * i + way, place(way, d + 1), e) for way in (0, 1)]

    def pass_on(i):
        for item in core_items(i):
            send_core(*item)

    def both_cores(i):
        for item in core_items(i):
            wait_core(*item)

    def turn(rows, hi_ref, lo_ref, at):
        hi, lo = split(jnp.concatenate(rows, axis=0).T)
        hi_ref[at] = hi
        lo_ref[at] = lo

    def prepare_own():
        @pl.loop(0, GL // GC)
        def _(k):
            at = pl.ds(pl.multiple_of(k * GC, GC), GC)
            for h in (0, 1):
                rows = [ost[part, quarter[i], at] for i in (2 * h, 2 * h + 1) for part in (0, 1)]
                turn(rows, pwh, pwl, (at, slice(h * N, (h + 1) * N)))

    def prepare_neighbour(h, lo, hi):
        for n, (i, first, last) in enumerate(PIECES):
            if i // 2 == h and lo <= first and last <= hi:
                crossing(n).wait_recv()

        @pl.loop(0, (hi - lo) // 2)
        def _(step):
            for k in (lo + 2 * step, lo + 2 * step + 1):
                at = pl.ds(pl.multiple_of(k * GC, GC), GC)
                rows = [nbst[i, part, :, at] for i in (2 * h, 2 * h + 1) for part in (0, 1)]
                turn(rows, pnh, pnl, (at, slice(h * N, (h + 1) * N)))

    R = 4 * M

    def three(hi, lo, right_hi, right_lo):
        rows = hi.shape[0]
        first = mm(jnp.concatenate([hi, lo], axis=0), right_hi)
        return first[:rows] + first[rows:] + mm(hi, right_lo)

    def named(blocks):
        return [(s, (xl + i) % 2) for s, i in blocks]

    def own_inner(*blocks):
        blocks = named(blocks)
        for s, e in blocks:

            @pl.loop(0, H // CC)
            def _(i):
                at = pl.ds(pl.multiple_of(i * CC, CC), CC)
                hi, lo = split(hb[s, e, :, :, :, at].reshape(R, CC))
                lbh[s, 0, e, :, at] = hi
                lbh[s, 1, e, :, at] = lo

        hi, lo = (jnp.concatenate([lbh[s, w, e] for s, e in blocks], axis=0) for w in (0, 1))
        product = three(hi, lo, pwh[0:H], pwl[0:H])
        for k, (s, e) in enumerate(blocks):
            acc_o[s, e] = product[k * R : (k + 1) * R]

    def own_outer(*blocks):
        blocks = named(blocks)
        for k, (s, e) in enumerate(blocks):

            @pl.loop(0, C // CC)
            def _(i):
                at = pl.ds(pl.multiple_of(i * CC, CC), CC)
                src = pl.ds(pl.multiple_of(H + i * CC, CC), CC)
                hi, lo = split(hb[s, e, :, :, :, src].reshape(R, CC))
                lbc[0, k, :, at] = hi
                lbc[1, k, :, at] = lo

        hi, lo = (lbc[w, : len(blocks)].reshape(-1, C) for w in (0, 1))
        product = three(hi, lo, pwh[H:GL], pwl[H:GL])
        for k, (s, e) in enumerate(blocks):
            acc_o[s, e] += product[k * R : (k + 1) * R]

    def own(*blocks):
        own_inner(*blocks)
        own_outer(*blocks)

    lane = lax.broadcasted_iota(jnp.int32, (2 * M, N), 1)
    def every(s):
        left = [lbh[s, w].reshape(2 * R, H) for w in (0, 1)]
        acc_n[s] = three(*left, pnh[...], pnl[...]).reshape(2, R, 2 * N)

    def half(s, h, lo, hi):
        k, at = slice(lo * GC, hi * GC), slice(h * N, (h + 1) * N)
        left = [lbh[s, w, :, :, k].reshape(2 * R, -1) for w in (0, 1)]
        acc_n[s, :, :, at] += three(*left, pnh[k, at], pnl[k, at]).reshape(2, R, N)

    def over(d, body):
        @pl.loop(0, 2 * d + 1)
        def _(i):
            body((z + NZ - d + i) % NZ)

    def pair(d, body):
        @pl.loop(0, 2)
        def _(i):
            body((z + NZ - d + 2 * d * i) % NZ)

    def y_copy(t, i, s):
        return remote(ys.at[t, i, s], yr.at[t, i, s], yss, yrs.at[(s // 4 + z // 4) % 2], to_y[i])

    def share(t, s, quarters=range(NY)):
        acc = (acc_o, acc_n)[t]
        real = lane % (2 * U) < U
        for h in sorted({i // 2 for i in quarters}):
            v = []
            for e in (0, 1):
                p = acc[s, e, :, h * N : (h + 1) * N].reshape(2, 2, M, N)
                p0, p1 = (p[:, w].reshape(2 * M, N) for w in (0, 1))
                crossed = jnp.where(real, pltpu.roll(p1, N - U, 1), pltpu.roll(p1, U, 1))
                v.append(crossed + jnp.where(real, p0, -p0))
            for i in (2 * h, 2 * h + 1):
                if i not in quarters:
                    continue
                if i % 2 == 0:
                    ys[t, i, s] = jnp.where(lane < N // 2, v[0], pltpu.roll(v[1], N // 2, 1))
                else:
                    ys[t, i, s] = jnp.where(lane < N // 2, pltpu.roll(v[0], N // 2, 1), v[1])
        for i in (1, 0, 2):
            if i in quarters:
                y_copy(t, i, s).start()

    loads[0].wait()
    loads[1].wait()
    send_z(0)
    send_core(0, z, 0)
    acc_n[...] = jnp.zeros_like(acc_n)
    loads[2].wait()
    loads[3].wait()
    prepare_own()

    for i, (_, dst) in enumerate(hx_parts):
        arrived(hb.at[z, nb, c, :, :, dst], xss.at[0], xrs.at[i], to_x)
    send_z(1)
    send_core(1, z, 1)
    send_psi(2, 4)
    wait_z(0)
    send_z(2)
    pass_on(0)

    wait_z(1)
    send_z(3)
    pass_on(1)
    send_psi(4, 5)
    wait_core(0, z, 0)
    wait_core(1, z, 1)
    own((z, 0), (z, 1))
    share(0, z)
    both_cores(0)
    own((place(0, 1), 0), (place(1, 1), 0))

    wait_z(2)
    send_z(4)
    pass_on(2)
    send_psi(5, 7)
    both_cores(1)
    own((place(0, 1), 1), (place(1, 1), 1))
    pair(1, lambda s: share(0, s))

    def first_half(s):
        half(s, 0, 0, Q)
        share(1, s, (0, 1))

    wait_z(3)
    send_z(5)
    pass_on(3)
    send_psi(7, len(PIECES))
    both_cores(2)
    own((place(0, 2), 0), (place(1, 2), 0))
    prepare_neighbour(0, 0, Q)
    over(1, first_half)

    wait_z(4)
    send_z(6)
    pass_on(4)
    both_cores(3)
    own((place(0, 2), 1), (place(1, 2), 1))
    pair(2, lambda s: share(0, s))
    pair(2, first_half)
    prepare_neighbour(1, 0, CUTS[1][1])
    over(2, lambda s: half(s, 1, 0, CUTS[1][1]))
    both_cores(4)
    own((place(0, 3), 0), (place(1, 3), 0))
    prepare_neighbour(1, CUTS[1][1], CUTS[1][2])
    over(2, lambda s: half(s, 1, CUTS[1][1], CUTS[1][2]))

    wait_z(5)
    send_z(7)
    send_z(8)
    pass_on(5)
    far = place(0, 4)
    last_items = ((14, far, 0), (15, far, 1, inner), (16, far, 1, outer))
    across = [cross(*item) for item in last_items]

    def finish(i):
        wait_z(6 + i)
        across[i].start()

    def on(core, *steps):
        @pl.when(c == core)
        def _():
            for step in steps:
                step()

    def at_turn(it, value, *steps):
        @pl.when(it == value)
        def _():
            for step in steps:
                step()

    def rest(s):
        half(s, 1, CUTS[1][2], Q)
        share(1, s, (2, 3))

    def end_of_psi():
        prepare_neighbour(1, CUTS[1][2], Q)
        over(2, rest)

    on(1, lambda: finish(0), end_of_psi)

    @pl.loop(0, 2)
    def _(it):
        blocks = ((jnp.where(it == 0, place(0, 3), far), 1 - it), (jnp.where(it == 0, place(1, 3), far), 1))

        def over_ready(body):
            @pl.loop(it, 2)
            def _(k):
                body(jnp.where(it == 1, far, jnp.where(k == 0, place(0, 3), place(1, 3))))

        def late(s):
            every(s)
            share(1, s)

        at_turn(it, 0, lambda: both_cores(5))
        at_turn(it, 1, lambda: on(1, lambda: finish(2)), *(lambda i=i: wait_core(*last_items[i]) for i in (0, 1)))
        own_inner(*blocks)
        at_turn(it, 0, lambda: on(0, end_of_psi, lambda: finish(0)))
        at_turn(it, 1, lambda: on(0, lambda: finish(2)))
        at_turn(it, 0, lambda: on(1, lambda: finish(1)))
        over_ready(late)
        at_turn(it, 1, lambda: wait_core(*last_items[2]))
        own_outer(*blocks)
        at_turn(it, 0, lambda: on(0, lambda: finish(1)))
        over_ready(lambda s: share(0, s))

    for turn_ in (0, 1):
        quad = z // 4 if turn_ == 0 else 1 - z // 4

        arrived(yr.at[:, :, pl.ds(0, 4)], yss, yrs.at[turn_], to_y[0])

        for t in (0, 1):
            rows = []
            for i in range(4):
                s = quad * 4 + i
                rows.append(ys[t, NY - 1, s] + yr[t, 0, s] + yr[t, 1, s] + yr[t, 2, s])
            block = jnp.concatenate(rows, axis=0).T.reshape(2, 2, 2, M, 128)
            for e in (0, 1):
                xt[turn_, t, :, :, :, e * 128 : (e + 1) * 128] = block[e]
        for k, (i, j) in enumerate(finals):
            copy = remote(
                xt.at[turn_, i, :, (xh + j) % 2], xr.at[turn_, k], fss, frs.at[turn_], to_f[k]
            )
            copy.start()
    for turn_ in (0, 1):
        quad = z // 4 if turn_ == 0 else 1 - z // 4
        total = xt[turn_, 0, :, xh]
        arrived(xr.at[turn_], fss, frs.at[turn_], to_f[0])
        for k in range(3):
            total = total + xr[turn_, k]
        for e in (0, 1):
            out[:, :, pl.ds(pl.multiple_of(e * 256 + quad * 128, 128), 128)] = total[:, :, e * 128 : (e + 1) * 128]

    for ref, sem in (
        (hb.at[pl.ds(0, 7), 0], zss),
        (hb.at[:, 0], dss),
        (hb.at[0, 0, 0], xss.at[0]),
        (nbst, xss.at[1]),
        (yr, yss),
        (xr, fss),
    ):
        remote(ref, ref, sem, sem, to_x).wait_send()


def per_device(psi, hx):
    f32, bf16, vmem, dma = jnp.float32, jnp.bfloat16, pltpu.VMEM, pltpu.SemaphoreType.DMA
    hbm = pl.BlockSpec(memory_space=pl.ANY)
    return pl.pallas_call(
        kernel,
        out_shape=pltpu.VMEM((2, N // 8, 32 * M), f32),
        in_specs=[hbm, hbm],
        out_specs=pl.BlockSpec(memory_space=pltpu.VMEM),
        scratch_shapes=[
            vmem((NZ, 2, 2, 2, M, GL), f32),
            vmem((NZ, 2, 2, 4 * M, H), bf16),
            vmem((2, 2, 4 * M, C), bf16),
            vmem((GL, 2 * N), bf16),
            vmem((GL, 2 * N), bf16),
            vmem((H, 2 * N), bf16),
            vmem((H, 2 * N), bf16),
            vmem((NY, 2, U, H), f32),
            vmem((2, N, GL), f32),
            vmem((NZ, 2, 4 * M, 2 * N), f32),
            vmem((NZ, 2, 4 * M, 2 * N), f32),
            vmem((2, NY, NZ, 2 * M, N), f32),
            vmem((2, NY - 1, NZ, 2 * M, N), f32),
            vmem((2, 2, 2, 2, M, 16 * M), f32),
            vmem((2, 3, 2, M, 16 * M), f32),
            dma((4,)),
            dma, dma((2, 9)),
            dma, dma((17,)),
            dma((2,)), dma((2 + len(PIECES),)),
            dma, dma((2,)),
            dma, dma((2,)),
        ],
        compiler_params=pltpu.CompilerParams(
            collective_id=0, has_side_effects=True, vmem_limit_bytes=66_000_000
        ),
    )(psi, hx)


def solution(mesh):
    in_specs = (P(None, "band", "ga"), P(None, "band", "ga"))
    out_specs = P(None, ("band", "ga"), None)
    return jax.shard_map(
        per_device, mesh=mesh, in_specs=in_specs, out_specs=out_specs, check_vma=False
    )
```
